256 devices in a mesh: rep: 16 (over x_hi, z), exp: 4 (over y), shard: 4 (over x_lo, core).
Axes of the slice: x: 4 (x_hi: 2, x_lo: 2; x = x_hi * 2 + x_lo), y: 4, z: 8, core: 2. Of those that a mesh axis runs over, the one named last changes fastest.
Arguments:
- deltas: bfloat16 [16, 4, 2048, 7168], P('rep', 'exp', 'shard'), may hold values from -0.1875 to 0.1875
- master: float32 [4, 2048, 7168], P('exp', 'shard', 'rep'), may hold values from -0.125 to 0.125
- momentum: float32 [4, 2048, 7168], P('exp', 'shard', 'rep'), may hold values from -0.12 to 0.12
- tokens: bfloat16 [4, 2048, 2048], P('exp', 'shard'), may hold values from -6 to 6
Outputs:
- new_master: float32 [4, 2048, 7168], P('exp', 'shard', 'rep')
- new_momentum: float32 [4, 2048, 7168], P('exp', 'shard', 'rep')
- probe_out: bfloat16 [4, 2048, 7168], P('exp', 'shard', 'rep')
The draws below stay inside these ranges and needn't reach their ends.
All inputs are finite; a program needn't handle non-finite values.
Results may differ from the reference program's by a relative error of at most 0.014.
Values may be sent and summed in bfloat16 or wider, within the bound.
No kernel may reach another device: no remote copies, remote signals or barrier semaphores. Data moves between devices by JAX's collectives and lax.ppermute only.
A program may use at most 128 MiB of HBM per device.

```python
import jax
import jax.numpy as jnp
from jax import lax

DW = 2048
FW = 7168
EXPERTS = 4
TOKENS = 2048
N_REP = 16


def strengthened(drawn, own_key, source, target, parts, factor):
    owner, partner = [(jnp.arange(drawn.shape[axis_at]) // (drawn.shape[axis_at] // parts)).reshape([-1 if axis == axis_at else 1 for axis in range(drawn.ndim)]) for axis_at in (source, target)]
    chosen = jax.random.permutation(own_key, parts)[partner]
    strong = (owner == chosen) | (owner == (partner + parts // 2) % parts)
    return jnp.where(strong, factor * drawn, drawn)


def block_levels(rng, shape, shards, smallest, top_value):
    loudness = 1.0
    for axis_at, blocks in shards:
        steps = jax.random.uniform(jax.random.fold_in(jax.random.fold_in(rng, 6), axis_at), (blocks,), jnp.float32, smallest / len(shards), top_value / len(shards))
        loudness = loudness * jnp.repeat(jnp.exp(steps), shape[axis_at] // blocks).reshape((-1,) + (1,) * (len(shape) - 1 - axis_at))
    return loudness


def scatter_about(key, extent, deviation, most, shards=(), kind=jnp.bfloat16):
    factor_of = block_levels(key, extent, shards, -0.22, 0.18) if shards else 1.0
    values = jax.random.normal(key, extent, jnp.float32) * deviation * factor_of
    return jnp.minimum(jnp.maximum(values, -most), most).astype(kind)


def bell_draw_with(own_key, dims, spread, reach, cuts, heavy, kind=jnp.bfloat16):
    entries = spread * jax.random.normal(own_key, dims, jnp.float32)
    if cuts:
        entries = entries * block_levels(own_key, dims, cuts, -0.22, 0.18)
    return jnp.clip(strengthened(entries, jax.random.fold_in(own_key, 3), *heavy), -reach, reach).astype(kind)


def setup_inputs(seed: int = 0) -> dict:
    key_list = jax.random.split(jax.random.key(seed), 5)
    deltas = bell_draw_with(key_list[0], (N_REP, EXPERTS, DW, FW), DW ** -0.5, 0.1875, ((0, 16), (1, 4), (2, 4)), (0, 3, 16, 2.0))
    master = scatter_about(key_list[1], (EXPERTS, DW, FW), DW ** -0.5, 0.125, ((0, 4), (1, 4), (2, 16)), jnp.float32)
    momentum = scatter_about(key_list[2], (EXPERTS, DW, FW), 0.02, 0.12, ((0, 4), (1, 4), (2, 16)), jnp.float32)
    tokens = scatter_about(key_list[3], (EXPERTS, TOKENS, DW), 1.0, 6.0, ((0, 4), (1, 4)))
    return {"deltas": deltas, "master": master, "momentum": momentum, "tokens": tokens}


outer_rate = 0.7
momentum_coef = 0.9


def reference(deltas, master, momentum, tokens):
    def accumulate(running, delta_one):
        return running + delta_one.astype(jnp.float32), None

    start_sum = jnp.zeros(master.shape, jnp.float32)
    summed, unused = lax.scan(accumulate, start_sum, deltas)
    outer_grad = summed / N_REP
    new_momentum = momentum_coef * momentum + outer_grad
    new_master = master - outer_rate * (outer_grad + momentum_coef * new_momentum)
    weight_bf = new_master.astype(jnp.bfloat16)
    probe_out = jnp.einsum("etd,edf->etf", tokens.astype(jnp.float32), weight_bf.astype(jnp.float32))
    return new_master, new_momentum, probe_out.astype(jnp.bfloat16)
```

```python
import functools

import jax
import jax.numpy as jnp
from jax import lax
from jax.experimental import pallas as pl
from jax.experimental.pallas import tpu as pltpu
from jax.sharding import Mesh
from jax.sharding import PartitionSpec as P


outer_rate = 0.7
momentum_coef = 0.9
NZ = 8
WIDE = 448
ALPHA = 192
BETA = WIDE - ALPHA
ROWS = 512
WINDOW = 512
LANES = 128
VMEM = pl.BlockSpec(memory_space=pltpu.VMEM)
ANY = pl.BlockSpec(memory_space=pl.ANY)
f32 = jnp.float32
bf16 = jnp.bfloat16


def shaped(rows, dtype=bf16):
    return jax.ShapeDtypeStruct((rows, ROWS), dtype)


def call(kernel, outs, ins, scratch=(), mib=2, out_specs=None):
    return pl.pallas_call(
        kernel,
        out_shape=outs,
        in_specs=ins,
        out_specs=out_specs or [VMEM] * len(outs),
        scratch_shapes=list(scratch),
        compiler_params=pltpu.CompilerParams(vmem_limit_bytes=mib * 1024 * 1024),
    )


def turned_kernel(k, deltas, after, a_ref, b_ref, c_ref, windows, whole, sems):
    del after
    xh, z, sh = (lax.axis_index(a) for a in ("xh", "z", "shard"))
    sign = 1 - 2 * lax.rem(sh, 2)
    zb = lax.rem(z - sign * (1 + k) + 2 * NZ, NZ)
    copies = []
    for n, x in enumerate((1 - xh, xh)):
        first = lax.div(WIDE * (x * NZ + zb), LANES)
        start = pl.multiple_of(first * LANES, LANES)
        copies.append(
            pltpu.make_async_copy(
                deltas.at[:, pl.ds(start, WINDOW)], windows.at[n], sems.at[n]
            )
        )
        copies[-1].start()
    for n in range(2):
        copies[n].wait()

        @pl.loop(0, WINDOW // LANES)
        def _(i, n=n):
            at = pl.multiple_of(i * LANES, LANES)
            whole[n, pl.ds(at, LANES), :] = windows[n, :, pl.ds(at, LANES)].T

    first = pl.multiple_of(64 * lax.rem(zb, 2), 64)
    a_ref[0:ALPHA] = whole[0, pl.ds(first, ALPHA), :]
    a_ref[ALPHA : 2 * ALPHA] = whole[1, pl.ds(first, ALPHA), :]
    second = pl.multiple_of(first + ALPHA, 64)
    c_ref[...] = whole[0, pl.ds(second, BETA), :]
    b_ref[...] = whole[1, pl.ds(second, BETA), :]


def turned(deltas, k, after):
    return call(
        functools.partial(turned_kernel, k),
        [shaped(2 * ALPHA), shaped(BETA), shaped(BETA)],
        [ANY, ANY],
        [
            pltpu.VMEM((2, ROWS, WINDOW), bf16),
            pltpu.VMEM((2, WINDOW, ROWS), bf16),
            pltpu.SemaphoreType.DMA((2,)),
        ],
        mib=5,
    )(deltas, after)


def sum_kernel(*refs):
    refs[-1][...] = sum(r[...].astype(f32) for r in refs[:-1]).astype(bf16)


def added(*terms):
    return call(sum_kernel, [shaped(terms[0].shape[0])], [VMEM] * len(terms))(*terms)[0]


def split_sum_kernel(x, y, far, near):
    far[...] = (x[0:ALPHA].astype(f32) + y[0:ALPHA].astype(f32)).astype(bf16)
    near[...] = x[ALPHA:].astype(f32) + y[ALPHA:].astype(f32)


def weight_kernel(rows, count, *refs):
    terms, (mas, mom, w, total, mas_v, mom_v, sems) = refs[:count], refs[count:]
    loads = [
        pltpu.make_async_copy(src.at[pl.ds(rows.start, rows.stop - rows.start)], dst, sems.at[i])
        for i, (src, dst) in enumerate(((mas, mas_v), (mom, mom_v)))
    ]
    for load in loads:
        load.start()
    total[...] = sum(t[...].astype(f32) for t in terms)
    for load in loads:
        load.wait()
    grad = total[...] / 16
    new_mom = momentum_coef * mom_v[...] + grad
    w[...] = (mas_v[...] - outer_rate * (grad + momentum_coef * new_mom)).astype(bf16)


def weight(rows, terms, mas, mom):
    n = rows.stop - rows.start
    return call(
        functools.partial(weight_kernel, rows, len(terms)),
        [shaped(n), shaped(n, f32)],
        [VMEM] * len(terms) + [ANY, ANY],
        [pltpu.VMEM((n, ROWS), f32), pltpu.VMEM((n, ROWS), f32), pltpu.SemaphoreType.DMA((2,))],
        mib=3,
    )(*terms, mas, mom)


def update_kernel(a, b, mas, mom, new_mas, new_mom):
    def write(total):
        grad = total / 16
        m = momentum_coef * mom[...] + grad
        new_mom[...] = m
        new_mas[...] = mas[...] - outer_rate * (grad + momentum_coef * m)

    i = pl.program_id(0)

    @pl.when(i < ALPHA // 64)
    def _():
        write(a[...])

    @pl.when(i >= ALPHA // 64)
    def _():
        write(b[...])


def updated(a, b, mas, mom):
    na = ALPHA // 64
    block = pl.BlockSpec((64, ROWS), lambda i: (i, 0))
    return pl.pallas_call(
        update_kernel,
        grid=(WIDE // 64,),
        out_shape=[shaped(WIDE, f32)] * 2,
        in_specs=[
            pl.BlockSpec((64, ROWS), lambda i: (jnp.minimum(i, na - 1), 0)),
            pl.BlockSpec((64, ROWS), lambda i: (jnp.maximum(i - na, 0), 0)),
            block,
            block,
        ],
        out_specs=[block] * 2,
        compiler_params=pltpu.CompilerParams(vmem_limit_bytes=4 * 1024 * 1024),
        name="update",
    )(a, b, mas, mom)


def tokens_kernel(tokens, out, sems):
    sh = lax.axis_index("shard")
    loads = []
    for j, bits in enumerate((0, 1, 2, 3)):
        there = sh + bits - 2 * (sh & bits)
        start = pl.multiple_of(there * ROWS, ROWS)
        loads.append(
            pltpu.make_async_copy(tokens.at[:, pl.ds(start, ROWS)], out.at[j], sems.at[j])
        )
        loads[-1].start()
    for load in loads:
        load.wait()


def dotted(w, t):
    return lax.dot_general(w, t, (((1,), (1,)), ((), ())), preferred_element_type=f32)


def near_kernel(w0, w1, tokens, out):
    out[...] = dotted(w0[...], tokens[0]) + dotted(w1[...], tokens[1])


def far_kernel(part, w2, w3, tokens, out):
    out[...] = (part[...] + dotted(w2[...], tokens[2]) + dotted(w3[...], tokens[3])).astype(bf16)


def last_kernel(head, part, w2, w3, tokens, out):
    out[0:ALPHA] = head[...]
    out[ALPHA:] = (part[...] + dotted(w2[...], tokens[2]) + dotted(w3[...], tokens[3])).astype(bf16)


def body(deltas, master, momentum, tokens):
    deltas = deltas[0, 0]
    mas, mom = master[0].T, momentum[0].T
    ring = [
        (4 * i + j, 4 * ((i + 1 - 2 * (j % 2)) % NZ) + j) for i in range(NZ) for j in range(4)
    ]

    def along_z(x):
        return lax.ppermute(x, ("z", "shard"), ring)

    def across_x(x):
        return lax.ppermute(x, "xh", [(0, 1), (1, 0)])

    def shard_swap(x, bit):
        return lax.ppermute(x, "shard", [(i, i ^ bit) for i in range(4)])

    own_a, own_b, swapped = {}, {}, {}

    def prepare(k, after):
        own_a[k], own_b[k], theirs = turned(deltas, k, after)
        swapped[k] = across_x(theirs)

    prepare(0, deltas)
    a = own_a[0]
    b = None
    for s in range(8):
        if s == 7:
            far_a, near_a = call(
                split_sum_kernel, [shaped(ALPHA), shaped(ALPHA, f32)], [VMEM] * 2
            )(a, own_a[7])
            far_a = across_x(far_a)
        else:
            if s:
                a = added(a, own_a[s])
            prepare(s + 1, a)
            a = along_z(a)
        if s:
            k = s - 1
            terms = [own_b[k], swapped[k]] + ([b] if k else [])
            b = along_z(added(*terms))

    wa, sum_a = weight(slice(0, ALPHA), (far_a, near_a), mas, mom)
    fara = shard_swap(wa, 2)
    besidea = shard_swap(wa, 1)
    wb, sum_b = weight(slice(ALPHA, WIDE), (b, own_b[7], swapped[7]), mas, mom)
    farb = shard_swap(wb, 2)
    besideb = shard_swap(wb, 1)
    new_master, new_momentum = updated(sum_a, sum_b, mas, mom)
    turned_tokens = call(
        tokens_kernel,
        [jax.ShapeDtypeStruct((4, ROWS, ROWS), bf16)],
        [ANY],
        [pltpu.SemaphoreType.DMA((4,))],
    )(tokens[0])[0]
    part_a = call(near_kernel, [shaped(ALPHA, f32)], [VMEM] * 3)(wa, besidea, turned_tokens)[0]
    part_b = call(near_kernel, [shaped(BETA, f32)], [VMEM] * 3)(wb, besideb, turned_tokens)[0]
    far_besidea = shard_swap(fara, 1)
    far_besideb = shard_swap(farb, 1)
    head = call(far_kernel, [shaped(ALPHA)], [VMEM] * 4)(
        part_a, fara, far_besidea, turned_tokens
    )[0]
    probe = call(last_kernel, [shaped(WIDE)], [VMEM] * 5)(
        head, part_b, farb, far_besideb, turned_tokens
    )[0]
    return new_master.T[None], new_momentum.T[None], probe.T[None]


def solution(mesh):
    torus = Mesh(
        mesh.devices.reshape(2, NZ, mesh.shape["exp"], mesh.shape["shard"]),
        ("xh", "z", "exp", "shard"),
    )
    rep = ("xh", "z")

    return jax.shard_map(
        body,
        mesh=torus,
        in_specs=(
            P(rep, "exp", "shard", None),
            P("exp", "shard", rep),
            P("exp", "shard", rep),
            P("exp", "shard", None),
        ),
        out_specs=(P("exp", "shard", rep),) * 3,
        check_vma=False,
    )
```

```python
import functools

import jax
import jax.numpy as jnp
from jax import lax
from jax.experimental import pallas as pl
from jax.experimental.pallas import tpu as pltpu
from jax.sharding import Mesh
from jax.sharding import PartitionSpec as P


outer_rate = 0.7
momentum_coef = 0.9
NZ = 8
WIDE = 448
ALPHA = 192
BETA = WIDE - ALPHA
ROWS = 512
WINDOW = 512
GROUPS = ((0, (1,)), (1, (2,)), (2, (3, 4)), (3, (5, 6)), (4, (7,)))
LANES = 128
VMEM = pl.BlockSpec(memory_space=pltpu.VMEM)
ANY = pl.BlockSpec(memory_space=pl.ANY)
HBM = pl.BlockSpec(memory_space=pltpu.HBM)
f32 = jnp.float32
bf16 = jnp.bfloat16


def shaped(rows, dtype=bf16):
    return jax.ShapeDtypeStruct((rows, ROWS), dtype)


def call(kernel, outs, ins, scratch=(), mib=2, out_specs=None):
    return pl.pallas_call(
        kernel,
        out_shape=outs,
        in_specs=ins,
        out_specs=out_specs or [VMEM] * len(outs),
        scratch_shapes=list(scratch),
        compiler_params=pltpu.CompilerParams(vmem_limit_bytes=mib * 1024 * 1024),
    )


def turned_kernel(k, half, extra, deltas, *refs):
    p_ref, o_ref, b_ref, c_ref, windows, whole, sems = refs[extra:]
    xh, z, sh = (lax.axis_index(a) for a in ("xh", "z", "shard"))
    sign = 1 - 2 * lax.rem(sh, 2)
    zb = lax.rem(z - sign * (1 + k) + 2 * NZ, NZ)
    copies = []
    for n, x in enumerate((1 - xh, xh)):
        first = lax.div(WIDE * (x * NZ + zb), LANES)
        start = pl.multiple_of(first * LANES, LANES)
        copies.append(
            pltpu.make_async_copy(
                deltas.at[:, pl.ds(start, WINDOW)], windows.at[n], sems.at[n]
            )
        )
        copies[-1].start()
    first = pl.multiple_of(64 * lax.rem(zb, 2), 64)
    second = pl.multiple_of(first + ALPHA, 16)
    for n, (a_ref, rest_ref, at_row) in enumerate(
        ((p_ref, c_ref, BETA * half), (o_ref, b_ref, 0))
    ):
        copies[n].wait()

        @pl.loop(0, WINDOW // LANES)
        def _(t, n=n):
            at = pl.multiple_of(t * LANES, LANES)
            whole[n, pl.ds(at, LANES), :] = windows[n, :, pl.ds(at, LANES)].T

        a_ref[...] = whole[n, pl.ds(first, ALPHA), :]
        rest_ref[at_row : at_row + BETA] = whole[n, pl.ds(second, BETA), :]


def turned(deltas, k, after, crossing, size):
    extras = [x for x in (after, crossing) if x is not None]
    half = 0 if crossing is None else 1
    return pl.pallas_call(
        functools.partial(turned_kernel, k, half, len(extras)),
        out_shape=[shaped(ALPHA), shaped(ALPHA), shaped(BETA), shaped(BETA * size)],
        in_specs=[HBM if k == 0 else ANY] + [ANY] * len(extras[: len(extras) - half]) + [VMEM] * half,
        out_specs=[VMEM] * 4,
        input_output_aliases={len(extras): 3} if half else {},
        scratch_shapes=[
            pltpu.VMEM((2, ROWS, WINDOW), bf16),
            pltpu.VMEM((2, WINDOW, ROWS), bf16),
            pltpu.SemaphoreType.DMA((2,)),
        ],
        compiler_params=pltpu.CompilerParams(vmem_limit_bytes=5 * 1024 * 1024),
    )(deltas, *extras)


def total_of(refs, part, rows):
    total = 0.0
    for i, r in enumerate(refs):
        at = part[1] if part and part[0] == i else 0
        total = total + r[at : at + rows].astype(f32)
    return total


def sum_kernel(part, *refs):
    refs[-1][...] = total_of(refs[:-1], part, refs[-1].shape[0]).astype(bf16)


def added(*terms, part=None):
    kernel = functools.partial(sum_kernel, part)
    return call(kernel, [shaped(terms[0].shape[0])], [VMEM] * len(terms))(*terms)[0]


def weight_kernel(rows, count, part, *refs):
    terms, (mas, mom, w, total, mas_v, mom_v, sems) = refs[:count], refs[count:]
    loads = [
        pltpu.make_async_copy(src.at[pl.ds(rows.start, rows.stop - rows.start)], dst, sems.at[i])
        for i, (src, dst) in enumerate(((mas, mas_v), (mom, mom_v)))
    ]
    for load in loads:
        load.start()
    total[...] = total_of(terms, part, total.shape[0])
    for load in loads:
        load.wait()
    grad = total[...] / 16
    new_mom = momentum_coef * mom_v[...] + grad
    w[...] = (mas_v[...] - outer_rate * (grad + momentum_coef * new_mom)).astype(bf16)


def weight(rows, terms, mas, mom, part=None):
    n = rows.stop - rows.start
    return call(
        functools.partial(weight_kernel, rows, len(terms), part),
        [shaped(n), shaped(n, f32)],
        [VMEM] * len(terms) + [ANY, ANY],
        [pltpu.VMEM((n, ROWS), f32), pltpu.VMEM((n, ROWS), f32), pltpu.SemaphoreType.DMA((2,))],
        mib=3,
    )(*terms, mas, mom)


def update_kernel(a, b, mas, mom, new_mas, new_mom):
    for total, rows in ((a, slice(0, ALPHA)), (b, slice(ALPHA, WIDE))):
        grad = total[...] / 16
        m = momentum_coef * mom[rows] + grad
        new_mom[rows] = m
        new_mas[rows] = mas[rows] - outer_rate * (grad + momentum_coef * m)


def updated(a, b, mas, mom):
    def block(rows):
        return pl.BlockSpec((rows, LANES), lambda i: (0, i))

    return pl.pallas_call(
        update_kernel,
        grid=(ROWS // LANES,),
        out_shape=[shaped(WIDE, f32)] * 2,
        in_specs=[block(ALPHA), block(BETA), block(WIDE), block(WIDE)],
        out_specs=[block(WIDE)] * 2,
        compiler_params=pltpu.CompilerParams(vmem_limit_bytes=4 * 1024 * 1024),
        name="update",
    )(a, b, mas, mom)


def tokens_kernel(tokens, out, sems):
    sh = lax.axis_index("shard")
    loads = []
    for j, bits in enumerate((0, 1, 2, 3)):
        there = sh + bits - 2 * (sh & bits)
        start = pl.multiple_of(there * ROWS, ROWS)
        loads.append(
            pltpu.make_async_copy(tokens.at[:, pl.ds(start, ROWS)], out.at[j], sems.at[j])
        )
        loads[-1].start()
    for load in loads:
        load.wait()


def dotted(w, t):
    return lax.dot_general(w, t, (((1,), (1,)), ((), ())), preferred_element_type=f32)


def near_kernel(w0, w1, tokens, out):
    out[...] = dotted(w0[...], tokens[0]) + dotted(w1[...], tokens[1])


def far_kernel(part, w2, w3, tokens, out):
    out[...] = (part[...] + dotted(w2[...], tokens[2]) + dotted(w3[...], tokens[3])).astype(bf16)


def last_kernel(head, part, w2, w3, tokens, out):
    out[0:ALPHA] = head[...]
    out[ALPHA:] = (part[...] + dotted(w2[...], tokens[2]) + dotted(w3[...], tokens[3])).astype(bf16)


def body(deltas, master, momentum, tokens):
    deltas = deltas[0, 0]
    mas, mom = master[0].T, momentum[0].T
    ring = [
        (4 * i + j, 4 * ((i + 1 - 2 * (j % 2)) % NZ) + j) for i in range(NZ) for j in range(4)
    ]

    def along_z(x):
        return lax.ppermute(x, ("z", "shard"), ring)

    def across_x(x):
        return lax.ppermute(x, "xh", [(0, 1), (1, 0)])

    def shard_swap(x, bit):
        return lax.ppermute(x, "shard", [(i, i ^ bit) for i in range(4)])

    own_p, own_o, own_b, swapped = {}, {}, {}, {}

    def prepare(group, after, source):
        theirs = None
        for k in group:
            own_p[k], own_o[k], own_b[k], theirs = turned(
                source, k, after if theirs is None else None, theirs, len(group)
            )
        return theirs

    def cross(group, theirs):
        crossed = across_x(theirs)
        for i, k in enumerate(group):
            swapped[k] = crossed, BETA * i

    cross((0,), prepare((0,), None, pltpu.with_memory_space_constraint(deltas, pltpu.HBM)))
    p, o, b = own_p[0], own_o[0], None
    for s in range(8):
        if s:
            p = added(p, own_p[s])
            if s < 7:
                o = added(o, own_o[s])
        for slot, group in GROUPS:
            if slot == s:
                cross(group, prepare(group, o, deltas))
        if s < 7:
            p = along_z(p)
            o = along_z(o)
        else:
            p = across_x(p)
        if s:
            k = s - 1
            terms = [own_b[k], swapped[k][0]] + ([b] if k else [])
            b = along_z(added(*terms, part=(1, swapped[k][1])))

    wa, sum_a = weight(slice(0, ALPHA), (p, o, own_o[7]), mas, mom)
    wb, sum_b = weight(
        slice(ALPHA, WIDE), (own_b[7], swapped[7][0], b), mas, mom, (1, swapped[7][1])
    )
    fara = shard_swap(wa, 2)
    besidea = shard_swap(wa, 1)
    farb = shard_swap(wb, 2)
    besideb = shard_swap(wb, 1)
    new_master, new_momentum = updated(sum_a, sum_b, mas, mom)
    turned_tokens = call(
        tokens_kernel,
        [jax.ShapeDtypeStruct((4, ROWS, ROWS), bf16)],
        [ANY],
        [pltpu.SemaphoreType.DMA((4,))],
    )(tokens[0])[0]
    part_a = call(near_kernel, [shaped(ALPHA, f32)], [VMEM] * 3)(wa, besidea, turned_tokens)[0]
    part_b = call(near_kernel, [shaped(BETA, f32)], [VMEM] * 3)(wb, besideb, turned_tokens)[0]
    far_besidea = shard_swap(fara, 1)
    far_besideb = shard_swap(farb, 1)
    head = call(far_kernel, [shaped(ALPHA)], [VMEM] * 4)(
        part_a, fara, far_besidea, turned_tokens
    )[0]
    probe = call(last_kernel, [shaped(WIDE)], [VMEM] * 5)(
        head, part_b, farb, far_besideb, turned_tokens
    )[0]
    return new_master.T[None], new_momentum.T[None], probe.T[None]


def solution(mesh):
    torus = Mesh(
        mesh.devices.reshape(2, NZ, mesh.shape["exp"], mesh.shape["shard"]),
        ("xh", "z", "exp", "shard"),
    )
    rep = ("xh", "z")

    return jax.shard_map(
        body,
        mesh=torus,
        in_specs=(
            P(rep, "exp", "shard", None),
            P("exp", "shard", rep),
            P("exp", "shard", rep),
            P("exp", "shard", None),
        ),
        out_specs=(P("exp", "shard", rep),) * 3,
        check_vma=False,
    )
```
